32 devices in a mesh: grp: 4 (over z), loc: 8 (over y, x, core).
Axes of the slice: x: 2, y: 2, z: 4, core: 2. Of those that a mesh axis runs over, the one named last changes fastest.
Arguments:
- features: float32 [32768, 256], P(('grp', 'loc')), may hold values from -6 to 6
- hub_block: bfloat16 [128, 32768], P(None, ('grp', 'loc')), may hold values from -0.0625 to 0.0625
- hub_slot: int32 [128], P(('grp', 'loc')), may hold values from 0 to 1023, as said below
- neighbours: int32 [32768, 16], P(('grp', 'loc')), may hold values from 0 to 2047
- counts: int32 [32768], P(('grp', 'loc')), may hold values from 1 to 16
- halo_send: int32 [256, 128], P(('grp', 'loc')), may hold values from 0 to 1023
- weight: float32 [256, 256], replicated, may hold values from -0.375 to 0.375
- bias: float32 [256], replicated, may hold values from -3 to 3
Outputs:
- layer_out: float32 [32768, 256], P(('grp', 'loc'))
The draws below stay inside these ranges and needn't reach their ends.
Inputs may be any that keep to these rules, and one draw needn't show every extreme that they name: `hub_slot`: within each aligned block of 4 entries the values are distinct.
All inputs are finite; a program needn't handle non-finite values.
Results may differ from the reference program's by a relative error of at most 0.0003.
Values sent between devices are 32-bit elements; how exact they have to be, the bound alone decides.
A program may use at most 64 MiB of HBM per device.

```python
import jax
import jax.numpy as jnp
from jax import lax

F = 256
V_DEV = 1024
HUB_DEV = 4
K = 16
S = 128
V = 32768
HUB = 128
N_GRP = 4
N_LOC = 8
DEVICES = 32


def draw_hub_slot(key, part):
    owners = HUB // HUB_DEV
    keys = jax.random.split(jax.random.fold_in(key, 11), owners)
    picked = jax.vmap(lambda single: jax.random.permutation(single, V_DEV)[:HUB_DEV])(keys)
    return picked.reshape(-1).astype(jnp.int32)


def place_ends(array, stream_key, least, largest):
    shape = array.shape
    spot = [jax.random.randint(jax.random.fold_in(stream_key, axis), (), 0, shape[axis]) for axis in range(len(shape))]
    array = array.at[tuple(spot)].set(least)
    longest = shape.index(max(shape))
    spot[longest] = (spot[longest] + 1) % shape[longest]
    return array.at[tuple(spot)].set(largest)


def spiked(entries, own_key, source, target, blocks, factor):
    def block_of(position):
        return (jnp.arange(entries.shape[position]) // (entries.shape[position] // blocks)).reshape((-1,) + (1,) * (entries.ndim - 1 - position))

    first = jax.random.permutation(own_key, blocks)[block_of(target)]
    other_side = (block_of(target) + blocks // 2) % blocks
    return jnp.where((block_of(source) == first) | (block_of(source) == other_side), factor * entries, entries)


def block_levels(key, extent, cuts, low, top_value):
    def one(dim, shards_of):
        draws = jax.random.uniform(jax.random.fold_in(jax.random.fold_in(key, 6), dim), (shards_of,), jnp.float32, low / len(cuts), top_value / len(cuts))
        return jnp.repeat(jnp.exp(draws), extent[dim] // shards_of).reshape((-1,) + (1,) * (len(extent) - dim - 1))

    loudness = one(*cuts[0])
    for cut in cuts[1:]:
        loudness = loudness * one(*cut)
    return loudness


def centred(key, extent, width, bound, cuts=(), kind=jnp.bfloat16):
    array = jax.random.normal(key, extent, jnp.float32) * width
    if len(cuts) > 0:
        array = block_levels(key, extent, cuts, -0.22, 0.18) * array
    return jnp.clip(array, min=-bound, max=bound).astype(kind)


def heavy_noise(key, extent, deviation, most, cuts, heavy, kind=jnp.bfloat16):
    entries = deviation * jax.random.normal(key, extent, jnp.float32)
    if cuts:
        entries = entries * block_levels(key, extent, cuts, -0.22, 0.18)
    return jnp.clip(spiked(entries, jax.random.fold_in(key, 3), *heavy), -most, most).astype(kind)


def setup_inputs(seed: int = 0) -> dict:
    splits = jax.random.split(jax.random.key(seed), 9)
    return {
        "features": centred(splits[0], (V, F), 1.0, 6.0, ((0, 32),), jnp.float32),
        "hub_block": heavy_noise(splits[1], (HUB, V), V ** -0.5, 0.0625, ((1, 32),), (1, 0, 32, 2.75)),
        "hub_slot": draw_hub_slot(jax.random.fold_in(splits[8], 71), 0),
        "neighbours": place_ends(jax.random.randint(splits[3], (V, K), 0, V_DEV + N_LOC * S), jax.random.fold_in(splits[3], 1), 0, (V_DEV + N_LOC * S) - 1).astype(jnp.int32),
        "counts": place_ends(jax.random.randint(splits[4], (V,), 1, K + 1), jax.random.fold_in(splits[4], 1), 1, K).astype(jnp.int32),
        "halo_send": place_ends(jax.random.randint(splits[5], (DEVICES * N_LOC, S), 0, V_DEV), jax.random.fold_in(splits[5], 1), 0, V_DEV - 1).astype(jnp.int32),
        "weight": centred(splits[6], (F, F), F ** -0.5, 0.375, (), jnp.float32),
        "bias": centred(splits[7], (F,), 0.5, 3.0, (), jnp.float32),
    }


def reference(features, hub_block, hub_slot, neighbours, counts, halo_send, weight, bias):
    rounded = features.astype(jnp.bfloat16)
    hub_sum = jnp.dot(hub_block, rounded, preferred_element_type=jnp.float32)
    devices = N_GRP * N_LOC
    send_table = halo_send.reshape(devices, N_LOC, S)
    nbr_blocks = neighbours.reshape(devices, V_DEV, K)
    cnt_blocks = counts.reshape(devices, V_DEV)

    def one_device(device):
        group = device // N_LOC
        place = device % N_LOC
        peers = (group * N_LOC + jnp.arange(N_LOC)).astype(jnp.int32)
        sent_rows = send_table[peers, place]
        remote_ids = (peers[:, None] * V_DEV + sent_rows).reshape(-1)
        own_ids = (device * V_DEV + jnp.arange(V_DEV)).astype(jnp.int32)
        ids_table = jnp.concatenate([own_ids, remote_ids.astype(jnp.int32)])
        slots = nbr_blocks[device]
        gathered = features[ids_table[slots]]
        used = (jnp.arange(K)[None, :] < cnt_blocks[device][:, None]).astype(jnp.float32)
        summed = jnp.sum(gathered * used[:, :, None], axis=1)
        return summed / cnt_blocks[device].astype(jnp.float32)[:, None]

    low = lax.map(one_device, jnp.arange(devices).astype(jnp.int32)).reshape(-1, F)
    combined = features + low
    targets = (jnp.arange(HUB) // HUB_DEV).astype(jnp.int32) * V_DEV + hub_slot
    combined = combined.at[targets].add(hub_sum)
    result = jnp.dot(combined, weight, precision=lax.Precision.HIGHEST, preferred_element_type=jnp.float32) + bias
    return jnp.maximum(result, 0.0)
```

```python
import functools

import jax
import jax.numpy as jnp
from jax import lax
from jax.experimental import pallas as pl
from jax.experimental.pallas import tpu as pltpu
from jax.sharding import PartitionSpec as P

BF = jnp.bfloat16
F32 = jnp.float32
LANES = 128


def flip(index, mask, count):
    result = index
    bit = 1
    while bit < count:
        if mask & bit:
            result = result + bit * (1 - 2 * ((index // bit) % 2))
        bit *= 2
    return result


def send_order(count):
    far = [off for off in range(2, count) if bin(off >> 1).count("1") > 1]
    near = [off for off in range(2, count) if bin(off >> 1).count("1") == 1][::-1]
    order = []
    while far or near:
        if far:
            order.append(far.pop(0))
        if near:
            order.append(near.pop(0))
    return order + [1]


def dot(a, b):
    return jnp.dot(a, b, preferred_element_type=F32)


def dot_nt(a, b):
    return lax.dot_general(a, b, (((1,), (1,)), ((), ())), preferred_element_type=F32)


def split(x):
    high = x.astype(BF)
    return high, (x - high.astype(F32)).astype(BF)


def onehot(mask):
    return jnp.where(mask, 1.0, 0.0).astype(BF)


def iota(shape, dim):
    return lax.broadcasted_iota(jnp.int32, shape, dim)


def kernel(
    n_grp, n_loc,
    feat_ref, hub_ref, slot_ref, nbr_ref, cnt_ref, halo_ref, w_ref, bias_ref,
    out_ref,
    fh, fl, ph, pl_, base, acc, adj, codes, lows, outgoing, recv, part, part_in, spread, spread_in,
    inv, wh, wl,
    halo_s, halo_r, grp_s, grp_r, loc_s, loc_r,
):
    grp = lax.axis_index("grp")
    me = lax.axis_index("loc")
    rows, width = feat_ref.shape
    listed = halo_ref.shape[1]
    slots = nbr_ref.shape[0]
    hub_grp = hub_ref.shape[0] // n_grp
    hub_dev = slot_ref.shape[0]
    levels = rows // LANES + n_loc * listed // LANES
    per_block = 256 // slots
    blocks = rows // per_block

    barrier = pltpu.get_barrier_semaphore()
    for off in range(1, n_loc):
        pl.semaphore_signal(
            barrier, inc=1, device_id={"loc": flip(me, off, n_loc)}, device_id_type=pl.DeviceIdType.MESH
        )
    for off in range(1, n_grp):
        pl.semaphore_signal(
            barrier, inc=1, device_id={"grp": (grp + off) % n_grp}, device_id_type=pl.DeviceIdType.MESH
        )

    high, low = split(feat_ref[...])
    fh[...] = high
    fl[...] = low
    part[...] = dot(hub_ref[...], fh[...])

    def gather(peer):
        line = halo_ref[pl.ds(peer, 1), :]
        column = jnp.transpose(jnp.broadcast_to(line, (LANES, listed)).astype(F32)).astype(jnp.int32)
        lane = iota((listed, LANES), 1)
        pick = jnp.concatenate(
            [onehot(column == lane + tile * LANES) for tile in range(rows // LANES)], axis=1
        )
        return dot(pick, fh[...]) + dot(pick, fl[...])

    def halo_copy(off):
        return pltpu.make_async_remote_copy(
            src_ref=outgoing.at[off],
            dst_ref=recv.at[pl.ds(pl.multiple_of(me * listed, listed), listed)],
            send_sem=halo_s.at[off],
            recv_sem=halo_r.at[off],
            device_id={"loc": flip(me, off, n_loc)},
            device_id_type=pl.DeviceIdType.MESH,
        )

    def grp_copy(off):
        target = (grp + off) % n_grp
        return pltpu.make_async_remote_copy(
            src_ref=part.at[pl.ds(pl.multiple_of(target * hub_grp, hub_grp), hub_grp)],
            dst_ref=part_in.at[off],
            send_sem=grp_s.at[off],
            recv_sem=grp_r.at[off],
            device_id={"grp": target},
            device_id_type=pl.DeviceIdType.MESH,
        )

    def loc_copy(off):
        target = flip(me, off, n_loc)
        return pltpu.make_async_remote_copy(
            src_ref=spread.at[target],
            dst_ref=spread_in.at[off],
            send_sem=loc_s.at[off],
            recv_sem=loc_r.at[off],
            device_id={"loc": target},
            device_id_type=pl.DeviceIdType.MESH,
        )

    order = send_order(n_loc)
    outgoing[order[0]] = gather(flip(me, order[0], n_loc))
    pl.semaphore_wait(barrier, n_loc - 1 + n_grp - 1)
    halo_copy(order[0]).start()
    for off in range(1, n_grp):
        grp_copy(off).start()
    for off in order[1:]:
        outgoing[off] = gather(flip(me, off, n_loc))
        halo_copy(off).start()
    recv[pl.ds(pl.multiple_of(me * listed, listed), listed), :] = gather(me)

    slot = nbr_ref[...]
    used = iota((slots, rows), 0) < jnp.broadcast_to(cnt_ref[...], (slots, rows))
    level = jnp.where(used, lax.shift_right_logical(slot, 7), -16).astype(F32)
    place = jnp.where(used, slot & (LANES - 1), 0).astype(F32)
    spots = (iota((rows, 256), 0) % per_block) == (iota((rows, 256), 1) % per_block)
    repeat = onehot(iota((slots, 256), 1) // per_block == iota((slots, 256), 0))
    member = onehot(iota((blocks, rows), 1) // per_block == iota((blocks, rows), 0))

    def flatten(table):
        spread_out = dot(jnp.transpose(table).astype(BF), repeat)
        return dot(member, jnp.where(spots, spread_out, 0.0).astype(BF))

    codes[...] = flatten(level).astype(jnp.int32) * per_block + iota((blocks, 256), 1) % per_block
    lows[...] = flatten(place).astype(jnp.int32)
    inv[...] = 1.0 / jnp.transpose(jnp.broadcast_to(cnt_ref[...].astype(F32), (8, rows)))

    w_high, w_low = split(w_ref[...])
    wh[...] = w_high
    wl[...] = w_low

    def times_weight(x_high, x_low):
        return dot(x_high, wh[...]) + dot(x_low, wh[...]) + dot(x_high, wl[...])

    product = times_weight(fh[...], fl[...])
    base[...] = product + bias_ref[...]
    p_high, p_low = split(product)
    ph[...] = p_high
    pl_[...] = p_low

    group = 4

    def build(step, carry):
        for inner in range(group):
            block = step * group + inner
            code = codes[pl.ds(block, 1), :]
            spot = lows[pl.ds(block, 1), :]
            left = onehot(iota((levels * per_block, 256), 0) == code)
            right = onehot(iota((LANES, 256), 0) == spot)
            counted = dot_nt(left, right).astype(BF)
            at = pl.ds(pl.multiple_of(block * per_block, per_block), per_block)
            for tile in range(levels):
                adj[tile // 2, at, (tile % 2) * LANES:(tile % 2 + 1) * LANES] = counted[
                    tile * per_block:(tile + 1) * per_block
                ]
        return carry

    lax.fori_loop(0, blocks // group, build, 0)

    own = rows // 256
    total = dot(adj[0], ph[0:256]) + dot(adj[0], pl_[0:256])
    for chunk in range(1, own):
        at = slice(chunk * 256, (chunk + 1) * 256)
        total = total + dot(adj[chunk], ph[at]) + dot(adj[chunk], pl_[at])
    acc[...] = total

    for off in range(1, n_grp):
        grp_copy(off).wait_recv()
    group_sum = part[pl.ds(pl.multiple_of(grp * hub_grp, hub_grp), hub_grp), :]
    for off in range(1, n_grp):
        group_sum = group_sum + part_in[off]
    spread[...] = jnp.zeros_like(spread)
    for owner in range(n_loc):
        spread[owner, 0:hub_dev, :] = group_sum[owner * hub_dev:(owner + 1) * hub_dev]
    for off in range(1, n_loc):
        loc_copy(off).start()

    def take(chip_off):
        chip = flip(me // 2, chip_off, n_loc // 2)
        got = recv[pl.ds(pl.multiple_of(chip * 2 * listed, 2 * listed), 2 * listed), :]
        r_high, r_low = split(times_weight(*split(got)))
        counts_of = adj[own + chip]
        return dot(counts_of, r_high) + dot(counts_of, r_low)

    chips = [0]
    for off in order:
        if off // 2 not in chips:
            chips.append(off // 2)
    halo_copy(1).wait_recv()
    for chip_off in chips[:-1]:
        if chip_off > 0:
            halo_copy(2 * chip_off).wait_recv()
            halo_copy(2 * chip_off + 1).wait_recv()
        acc[...] += take(chip_off)

    hubs = spread[me]
    for off in range(1, n_loc):
        loc_copy(off).wait_recv()
        hubs = hubs + spread_in[off]
    hubs = jnp.concatenate([hubs, jnp.zeros((LANES - hubs.shape[0], width), F32)], axis=0)
    h_high, h_low = split(times_weight(*split(hubs)))
    lane = iota((1, LANES), 1)
    target_row = jnp.full((1, LANES), -1, jnp.int32)
    for hub in range(hub_dev):
        target_row = jnp.where(lane == hub, slot_ref[hub], target_row)
    here = onehot(iota((rows, LANES), 0) == target_row)
    base[...] += dot(here, h_high) + dot(here, h_low)

    last = chips[-1]
    halo_copy(2 * last).wait_recv()
    halo_copy(2 * last + 1).wait_recv()
    out_ref[...] = jnp.maximum((acc[...] + take(last)) * inv[:, 0:1] + base[...], 0.0)

    for off in range(1, n_loc):
        halo_copy(off).wait_send()
        loc_copy(off).wait_send()
    for off in range(1, n_grp):
        grp_copy(off).wait_send()


def solution(mesh):
    n_grp, n_loc = mesh.shape["grp"], mesh.shape["loc"]

    def on_device(features, hub_block, hub_slot, neighbours, counts, halo_send, weight, bias):
        rows, width = features.shape
        slots = neighbours.shape[1]
        listed = halo_send.shape[1]
        hubs = hub_block.shape[0]
        pool = rows + n_loc * listed
        blocks = rows // (256 // slots)
        padded = -(-hub_slot.shape[0] // 8) * 8
        vmem = pl.BlockSpec(memory_space=pltpu.VMEM)
        smem = pl.BlockSpec(memory_space=pltpu.SMEM)
        sem = pltpu.SemaphoreType.DMA
        return pl.pallas_call(
            functools.partial(kernel, n_grp, n_loc),
            out_shape=jax.ShapeDtypeStruct((rows, width), F32),
            in_specs=[vmem, vmem, smem, vmem, vmem, vmem, vmem, vmem],
            out_specs=vmem,
            scratch_shapes=[
                pltpu.VMEM((rows, width), BF),
                pltpu.VMEM((rows, width), BF),
                pltpu.VMEM((rows, width), BF),
                pltpu.VMEM((rows, width), BF),
                pltpu.VMEM((rows, width), F32),
                pltpu.VMEM((rows, width), F32),
                pltpu.VMEM((pool // 256, rows, 256), BF),
                pltpu.VMEM((blocks, 256), jnp.int32),
                pltpu.VMEM((blocks, 256), jnp.int32),
                pltpu.VMEM((n_loc, listed, width), F32),
                pltpu.VMEM((n_loc * listed, width), F32),
                pltpu.VMEM((hubs, width), F32),
                pltpu.VMEM((n_grp, hubs // n_grp, width), F32),
                pltpu.VMEM((n_loc, padded, width), F32),
                pltpu.VMEM((n_loc, padded, width), F32),
                pltpu.VMEM((rows, 8), F32),
                pltpu.VMEM(weight.shape, BF),
                pltpu.VMEM(weight.shape, BF),
                sem((n_loc,)), sem((n_loc,)), sem((n_grp,)), sem((n_grp,)), sem((n_loc,)), sem((n_loc,)),
            ],
            compiler_params=pltpu.CompilerParams(
                collective_id=0, has_side_effects=True, vmem_limit_bytes=48 * 1024 * 1024
            ),
        )(
            features, hub_block, hub_slot, neighbours.T, counts.reshape(1, -1), halo_send, weight,
            bias.reshape(1, -1),
        )

    both = ("grp", "loc")
    return jax.shard_map(
        on_device,
        mesh=mesh,
        in_specs=(P(both, None), P(None, both), P(both), P(both, None), P(both), P(both, None), P(), P()),
        out_specs=P(both, None),
        check_vma=False,
    )
```

```python
import functools

import jax
import jax.numpy as jnp
from jax import lax
from jax.experimental import pallas as pl
from jax.experimental.pallas import tpu as pltpu
from jax.sharding import PartitionSpec as P

BF = jnp.bfloat16
F32 = jnp.float32
LANES = 128


def flip(index, mask, count):
    result = index
    bit = 1
    while bit < count:
        if mask & bit:
            result = result + bit * (1 - 2 * ((index // bit) % 2))
        bit *= 2
    return result


def send_order(count):
    far = [off for off in range(2, count) if bin(off >> 1).count("1") > 1]
    near = [off for off in range(2, count) if bin(off >> 1).count("1") == 1][::-1]
    order = []
    while far or near:
        if far:
            order.append(far.pop(0))
        if near:
            order.append(near.pop(0))
    return order + [1]


def dot(a, b):
    return jnp.dot(a, b, preferred_element_type=F32)


def dot_nt(a, b):
    return lax.dot_general(a, b, (((1,), (1,)), ((), ())), preferred_element_type=F32)


def split(x):
    high = x.astype(BF)
    return high, (x - high.astype(F32)).astype(BF)


def onehot(mask):
    return jnp.where(mask, 1.0, 0.0).astype(BF)


def iota(shape, dim):
    return lax.broadcasted_iota(jnp.int32, shape, dim)


def kernel(
    n_grp, n_loc,
    feat_hbm, hub_hbm, slot_hbm, nbr_hbm, cnt_hbm, halo_hbm, w_hbm, bias_hbm,
    out_ref,
    feat_ref, hub_ref, slot_ref, nbr_ref, cnt_ref, halo_ref, w_ref, bias_ref, loaded,
    fh, fl, ph, pl_, base, acc, adj, codes, lows, outgoing, recv, part, part_in, spread, spread_in,
    inv, wh, wl,
    halo_s, halo_r, grp_s, grp_r, loc_s, loc_r,
):
    grp = lax.axis_index("grp")
    me = lax.axis_index("loc")
    rows, width = feat_ref.shape
    listed = halo_ref.shape[1]
    slots = nbr_ref.shape[0]
    hub_grp = hub_ref.shape[0] // n_grp
    hub_dev = slot_ref.shape[0]
    levels = rows // LANES + n_loc * listed // LANES
    per_block = 256 // slots
    blocks = rows // per_block

    barrier = pltpu.get_barrier_semaphore()
    for off in range(1, n_loc):
        pl.semaphore_signal(
            barrier, inc=1, device_id={"loc": flip(me, off, n_loc)}, device_id_type=pl.DeviceIdType.MESH
        )
    for off in range(1, n_grp):
        pl.semaphore_signal(
            barrier, inc=1, device_id={"grp": (grp + off) % n_grp}, device_id_type=pl.DeviceIdType.MESH
        )

    halo_load, feat_load, hub_load, nbr_load, cnt_load, w_load, bias_load, slot_load = [
        pltpu.make_async_copy(source, target, loaded.at[number])
        for number, (source, target) in enumerate((
            (halo_hbm, halo_ref), (feat_hbm, feat_ref), (hub_hbm, hub_ref), (nbr_hbm, nbr_ref),
            (cnt_hbm, cnt_ref), (w_hbm, w_ref), (bias_hbm, bias_ref), (slot_hbm, slot_ref),
        ))
    ]
    for load in (halo_load, feat_load, hub_load, nbr_load, cnt_load, w_load, bias_load, slot_load):
        load.start()
    halo_load.wait()
    feat_load.wait()
    high, low = split(feat_ref[...])
    fh[...] = high
    fl[...] = low

    def gather(peer):
        line = halo_ref[pl.ds(peer, 1), :]
        column = jnp.transpose(jnp.broadcast_to(line, (LANES, listed)).astype(F32)).astype(jnp.int32)
        lane = iota((listed, LANES), 1)
        pick = jnp.concatenate(
            [onehot(column == lane + tile * LANES) for tile in range(rows // LANES)], axis=1
        )
        return dot(pick, fh[...]) + dot(pick, fl[...])

    def halo_copy(off):
        return pltpu.make_async_remote_copy(
            src_ref=outgoing.at[off],
            dst_ref=recv.at[pl.ds(pl.multiple_of(me * listed, listed), listed)],
            send_sem=halo_s.at[off],
            recv_sem=halo_r.at[off],
            device_id={"loc": flip(me, off, n_loc)},
            device_id_type=pl.DeviceIdType.MESH,
        )

    def grp_copy(off):
        target = (grp + off) % n_grp
        return pltpu.make_async_remote_copy(
            src_ref=part.at[pl.ds(pl.multiple_of(target * hub_grp, hub_grp), hub_grp)],
            dst_ref=part_in.at[off],
            send_sem=grp_s.at[off],
            recv_sem=grp_r.at[off],
            device_id={"grp": target},
            device_id_type=pl.DeviceIdType.MESH,
        )

    def loc_copy(off):
        target = flip(me, off, n_loc)
        return pltpu.make_async_remote_copy(
            src_ref=spread.at[target],
            dst_ref=spread_in.at[off],
            send_sem=loc_s.at[off],
            recv_sem=loc_r.at[off],
            device_id={"loc": target},
            device_id_type=pl.DeviceIdType.MESH,
        )

    order = send_order(n_loc)
    outgoing[order[0]] = gather(flip(me, order[0], n_loc))
    pl.semaphore_wait(barrier, n_loc - 1 + n_grp - 1)
    halo_copy(order[0]).start()
    for number, off in enumerate(order[1:]):
        outgoing[off] = gather(flip(me, off, n_loc))
        halo_copy(off).start()
        if number == 0:
            hub_load.wait()
            part[...] = dot(hub_ref[...], fh[...])
            for grp_off in range(1, n_grp):
                grp_copy(grp_off).start()
    recv[pl.ds(pl.multiple_of(me * listed, listed), listed), :] = gather(me)

    nbr_load.wait()
    cnt_load.wait()
    slot = nbr_ref[...]
    used = iota((slots, rows), 0) < jnp.broadcast_to(cnt_ref[...], (slots, rows))
    level = jnp.where(used, lax.shift_right_logical(slot, 7), -16).astype(F32)
    place = jnp.where(used, slot & (LANES - 1), 0).astype(F32)
    spots = (iota((rows, 256), 0) % per_block) == (iota((rows, 256), 1) % per_block)
    repeat = onehot(iota((slots, 256), 1) // per_block == iota((slots, 256), 0))
    member = onehot(iota((blocks, rows), 1) // per_block == iota((blocks, rows), 0))

    def flatten(table):
        spread_out = dot(jnp.transpose(table).astype(BF), repeat)
        return dot(member, jnp.where(spots, spread_out, 0.0).astype(BF))

    codes[...] = flatten(level).astype(jnp.int32) * per_block + iota((blocks, 256), 1) % per_block
    lows[...] = flatten(place).astype(jnp.int32)
    inv[...] = 1.0 / jnp.transpose(jnp.broadcast_to(cnt_ref[...].astype(F32), (8, rows)))

    w_load.wait()
    bias_load.wait()
    w_high, w_low = split(w_ref[...])
    wh[...] = w_high
    wl[...] = w_low

    def times_weight(x_high, x_low):
        return dot(x_high, wh[...]) + dot(x_low, wh[...]) + dot(x_high, wl[...])

    product = times_weight(fh[...], fl[...])
    base[...] = product + bias_ref[...]
    p_high, p_low = split(product)
    ph[...] = p_high
    pl_[...] = p_low

    group = 4
    own = rows // 256

    def build(step, carry):
        for inner in range(group):
            block = step * group + inner
            code = codes[pl.ds(block, 1), :]
            spot = lows[pl.ds(block, 1), :]
            left = onehot(iota((levels * per_block, 256), 0) == code)
            right = onehot(iota((LANES, 256), 0) == spot)
            counted = dot_nt(left, right).astype(BF)
            at = pl.ds(pl.multiple_of(block * per_block, per_block), per_block)
            for tile in range(levels):
                piece = counted[tile * per_block:(tile + 1) * per_block]
                if tile < 2 * own:
                    adj[tile // 2, at, (tile % 2) * LANES:(tile % 2 + 1) * LANES] = piece
                else:
                    adj[tile - own, at, 0:LANES] = piece
                    adj[tile - own, at, LANES:2 * LANES] = piece
        return carry

    lax.fori_loop(0, blocks // group, build, 0)

    total = dot(adj[0], ph[0:256]) + dot(adj[0], pl_[0:256])
    for chunk in range(1, own):
        at = slice(chunk * 256, (chunk + 1) * 256)
        total = total + dot(adj[chunk], ph[at]) + dot(adj[chunk], pl_[at])
    acc[...] = total

    for off in range(1, n_grp):
        grp_copy(off).wait_recv()
    group_sum = part[pl.ds(pl.multiple_of(grp * hub_grp, hub_grp), hub_grp), :]
    for off in range(1, n_grp):
        group_sum = group_sum + part_in[off]
    spread[...] = jnp.zeros_like(spread)
    for owner in range(n_loc):
        spread[owner, 0:hub_dev, :] = group_sum[owner * hub_dev:(owner + 1) * hub_dev]
    for off in range(1, n_loc):
        loc_copy(off).start()

    def take(off):
        peer = flip(me, off, n_loc)
        got = recv[pl.ds(pl.multiple_of(peer * listed, listed), listed), :]
        r_high, r_low = split(times_weight(*split(got)))
        return dot(adj[own + peer], jnp.concatenate([r_high, r_low], axis=0))

    acc[...] += take(0)
    arrivals = [1] + order[:-1]
    for off in arrivals[:-1]:
        halo_copy(off).wait_recv()
        acc[...] += take(off)

    hubs = spread[me]
    for off in range(1, n_loc):
        loc_copy(off).wait_recv()
        hubs = hubs + spread_in[off]
    hubs = jnp.concatenate([hubs, jnp.zeros((LANES - hubs.shape[0], width), F32)], axis=0)
    h_high, h_low = split(times_weight(*split(hubs)))
    slot_load.wait()
    lane = iota((1, LANES), 1)
    target_row = jnp.full((1, LANES), -1, jnp.int32)
    for hub in range(hub_dev):
        target_row = jnp.where(lane == hub, slot_ref[hub], target_row)
    here = onehot(iota((rows, LANES), 0) == target_row)
    base[...] += dot(here, h_high) + dot(here, h_low)

    last = arrivals[-1]
    halo_copy(last).wait_recv()
    out_ref[...] = jnp.maximum((acc[...] + take(last)) * inv[:, 0:1] + base[...], 0.0)

    for off in range(1, n_loc):
        halo_copy(off).wait_send()
        loc_copy(off).wait_send()
    for off in range(1, n_grp):
        grp_copy(off).wait_send()


def solution(mesh):
    n_grp, n_loc = mesh.shape["grp"], mesh.shape["loc"]

    def on_device(features, hub_block, hub_slot, neighbours, counts, halo_send, weight, bias):
        rows, width = features.shape
        slots = neighbours.shape[1]
        listed = halo_send.shape[1]
        hubs = hub_block.shape[0]
        blocks = rows // (256 // slots)
        padded = -(-hub_slot.shape[0] // 8) * 8
        vmem = pl.BlockSpec(memory_space=pltpu.VMEM)
        far = pl.BlockSpec(memory_space=pltpu.HBM)
        sem = pltpu.SemaphoreType.DMA
        return pl.pallas_call(
            functools.partial(kernel, n_grp, n_loc),
            out_shape=jax.ShapeDtypeStruct((rows, width), F32),
            in_specs=[far] * 8,
            out_specs=vmem,
            scratch_shapes=[
                pltpu.VMEM(features.shape, F32),
                pltpu.VMEM(hub_block.shape, BF),
                pltpu.SMEM(hub_slot.shape, jnp.int32),
                pltpu.VMEM((slots, rows), jnp.int32),
                pltpu.VMEM((1, rows), jnp.int32),
                pltpu.VMEM(halo_send.shape, jnp.int32),
                pltpu.VMEM(weight.shape, F32),
                pltpu.VMEM((1, width), F32),
                sem((8,)),
                pltpu.VMEM((rows, width), BF),
                pltpu.VMEM((rows, width), BF),
                pltpu.VMEM((rows, width), BF),
                pltpu.VMEM((rows, width), BF),
                pltpu.VMEM((rows, width), F32),
                pltpu.VMEM((rows, width), F32),
                pltpu.VMEM((rows // 256 + n_loc, rows, 256), BF),
                pltpu.VMEM((blocks, 256), jnp.int32),
                pltpu.VMEM((blocks, 256), jnp.int32),
                pltpu.VMEM((n_loc, listed, width), F32),
                pltpu.VMEM((n_loc * listed, width), F32),
                pltpu.VMEM((hubs, width), F32),
                pltpu.VMEM((n_grp, hubs // n_grp, width), F32),
                pltpu.VMEM((n_loc, padded, width), F32),
                pltpu.VMEM((n_loc, padded, width), F32),
                pltpu.VMEM((rows, 8), F32),
                pltpu.VMEM(weight.shape, BF),
                pltpu.VMEM(weight.shape, BF),
                sem((n_loc,)), sem((n_loc,)), sem((n_grp,)), sem((n_grp,)), sem((n_loc,)), sem((n_loc,)),
            ],
            compiler_params=pltpu.CompilerParams(
                collective_id=0, has_side_effects=True, vmem_limit_bytes=48 * 1024 * 1024
            ),
        )(
            *[
                pltpu.with_memory_space_constraint(array, pltpu.HBM)
                for array in (
                    features, hub_block, hub_slot, neighbours.T, counts.reshape(1, -1), halo_send, weight,
                    bias.reshape(1, -1),
                )
            ]
        )

    both = ("grp", "loc")
    return jax.shard_map(
        on_device,
        mesh=mesh,
        in_specs=(P(both, None), P(None, both), P(both), P(both, None), P(both), P(both, None), P(), P()),
        out_specs=P(both, None),
        check_vma=False,
    )
```
